32 devices in a mesh: dp: 8 (over z, core), ctx: 4 (over y, x).
Axes of the slice: x: 2, y: 2, z: 4, core: 2. Of those that a mesh axis runs over, the one named last changes fastest.
Arguments:
- qkv: bfloat16 [8, 512, 5120], P('dp', 'ctx'), may hold values from -8 to 8
- dest: int32 [8, 8], P('dp'), may hold values from 0 to 7, as said below
- order: int32 [8], replicated, may hold values from 0 to 7, as said below
- lengths: int32 [8, 8], replicated, may hold values from 1 to 256, 512 in all within a row
Outputs:
- attended: bfloat16 [8, 512, 4096], P('dp', 'ctx')
The draws below stay inside these ranges and needn't reach their ends.
Inputs may be any that keep to these rules, and one draw needn't show every extreme that they name: `dest`: entry [r, s] is r itself, r + 1 or r - 1 (indices modulo 8), and the relation is mutual: if entry [r, s] is t, entry [t, s] is r. For every c below 4: order[2 c] is below 4 and order[2 c + 1] = 7 - order[2 c]; every span appears once.
All inputs are finite; a program needn't handle non-finite values.
Results may differ from the reference program's by a relative error of at most 0.0031.
Values may be sent and summed in bfloat16 or wider, within the bound.
A program may use at most 64 MiB of HBM per device.

```python
import math
import jax
import jax.numpy as jnp
import numpy as np
from jax import lax

QUERY_HEADS = 32
KEY_VALUE_HEADS = 4
HEAD_SIZE = 128
NDOC = 8
SPAN = 64
QUERIES_PER_KV = 8
WIDTH = 5120
PACKED_LENGTH = 512
MAXDOC = 256
PACKED_COUNT = 8
N_CTX = 4


def draw_dest(key, part):
    parity = jax.random.randint(jax.random.fold_in(key, 11), (2 * N_CTX,), 0, 2)
    flips = jax.random.randint(jax.random.fold_in(key, 12), (PACKED_COUNT, 2 * N_CTX), 0, 2)
    ranks = jnp.arange(PACKED_COUNT, dtype=jnp.int32)[:, None]
    is_lower = (ranks - parity[None, :]) % 2 == 0
    lower_member = jnp.where(is_lower, ranks, ranks - 1) % PACKED_COUNT
    partner = jnp.where(is_lower, ranks + 1, ranks - 1) % PACKED_COUNT
    traded = jnp.take_along_axis(flips, lower_member, axis=0)
    return jnp.where(traded == 1, partner, ranks * jnp.ones_like(partner)).astype(jnp.int32)


def draw_order(key, part):
    early = jax.random.permutation(jax.random.fold_in(key, 21), N_CTX).astype(jnp.int32)
    late = (2 * N_CTX - 1 - early).astype(jnp.int32)
    return jnp.stack([early, late], axis=1).reshape(2 * N_CTX).astype(jnp.int32)


def draw_qkv(key, part):
    random_keys = jax.random.split(jax.random.fold_in(key, 31), 1)
    blank_scores = jax.random.normal(random_keys[0], (PACKED_COUNT, PACKED_LENGTH, WIDTH), jnp.float32)
    return jnp.clip(blank_scores, -8.0, 8.0).astype(jnp.bfloat16)


def profile(number_of, total, most, skew):
    weights = [(1 << 20) // math.isqrt(rank ** skew) + 1 for rank in range(2, number_of + 1)]
    surplus, counts = total - most - (number_of - 1), [1] * (number_of - 1)
    while surplus > 0:
        free = [i for i in range(number_of - 1) if counts[i] < most]
        pool, left = sum([weights[i] for i in free]), surplus
        for i in free:
            addition = min(most - counts[i], max(1, left * weights[i] // pool), surplus)
            counts[i] = counts[i] + addition
            surplus = surplus - addition
    return np.array([most] + counts)


def uneven_parts(own_key, amount, total, limit, lean):
    if amount == 2:
        one = jax.random.randint(own_key, (), max(1, total - limit), min(limit, total - 1) + 1)
        return jnp.stack([one, total - one])
    sizes = jnp.asarray(profile(amount, total, limit, lean), jnp.int32)
    pairs = (amount - 1) // 2
    donor, taker = sizes[1:1 + 2 * pairs:2], sizes[2:2 + 2 * pairs:2]
    slack = jnp.minimum(donor - 1, limit - taker)
    passed = jax.random.randint(jax.random.fold_in(own_key, 1), (pairs,), 0, 1 << 20) % (slack + 1)
    sizes = sizes.at[1:1 + 2 * pairs:2].set(donor - passed).at[2:2 + 2 * pairs:2].set(taker + passed)
    return sizes[jax.random.permutation(jax.random.fold_in(own_key, 2), amount)]


def setup_inputs(seed: int = 0) -> dict:
    streams_of = jax.random.split(jax.random.key(seed), 5)
    qkv = draw_qkv(jax.random.fold_in(streams_of[4], 71), 0)
    dest = draw_dest(jax.random.fold_in(streams_of[4], 71), 0)
    order = draw_order(jax.random.fold_in(streams_of[4], 71), 0)
    lengths = jax.vmap(lambda own: uneven_parts(own, NDOC, PACKED_LENGTH, MAXDOC, 2))(jax.random.split(streams_of[3], PACKED_COUNT)).reshape((PACKED_COUNT, NDOC)).astype(jnp.int32)
    return dict(qkv=qkv, dest=dest, order=order, lengths=lengths)


MASK_FLOOR = -1e+30

def sequence_attention(qkv, dest, order, doc_ends, seq_index):
    row_ids = jnp.arange(PACKED_LENGTH, dtype=jnp.int32)
    row_slot = (row_ids // SPAN).astype(jnp.int32)
    dest_row = lax.dynamic_index_in_dim(dest, seq_index, 0, keepdims=False)
    row_source = jnp.take(dest_row, row_slot).astype(jnp.int32)
    settled = qkv[row_source, row_ids]
    positions = (jnp.take(order, row_slot) * SPAN + row_ids % SPAN).astype(jnp.int32)
    row_ends = jnp.take(doc_ends, row_source, axis=0)
    counted = lax.optimization_barrier(jnp.sum((row_ends <= positions[:, None]).astype(jnp.int32), axis=1))
    documents = (row_source * NDOC + counted).astype(jnp.int32)
    visible = (documents[None, :] == documents[:, None]) & (positions[None, :] <= positions[:, None])
    score_scale = 1.0 / math.sqrt(HEAD_SIZE)
    finished = []
    for head_group_index in range(KEY_VALUE_HEADS):
        query_cols = settled[:, head_group_index * QUERIES_PER_KV * HEAD_SIZE:(head_group_index + 1) * QUERIES_PER_KV * HEAD_SIZE]
        query_block = query_cols.reshape(PACKED_LENGTH, QUERIES_PER_KV, HEAD_SIZE).astype(jnp.float32)
        key_start = QUERY_HEADS * HEAD_SIZE + head_group_index * HEAD_SIZE
        value_offset = (QUERY_HEADS + KEY_VALUE_HEADS) * HEAD_SIZE + head_group_index * HEAD_SIZE
        key_block = settled[:, key_start:key_start + HEAD_SIZE].astype(jnp.float32)
        value_block = settled[:, value_offset:value_offset + HEAD_SIZE].astype(jnp.float32)
        scores = jnp.einsum('qgd,kd->gqk', query_block, key_block, precision=lax.Precision.HIGHEST) * score_scale
        scores = jnp.where(visible[None], scores, MASK_FLOOR)
        row_max = lax.optimization_barrier(jnp.max(scores, axis=2, keepdims=True))
        weights = jnp.where(visible[None], jnp.exp(scores - row_max), 0.0)
        totals = lax.optimization_barrier(jnp.sum(weights, axis=2, keepdims=True))
        rounded = weights.astype(jnp.bfloat16).astype(jnp.float32)
        mixed = jnp.einsum('gqk,kd->gqd', rounded, value_block, precision=lax.Precision.HIGHEST) / totals
        finished.append(jnp.transpose(mixed, (1, 0, 2)).reshape(PACKED_LENGTH, QUERIES_PER_KV * HEAD_SIZE))
    return jnp.concatenate(finished, axis=1).astype(jnp.bfloat16)

def reference(qkv, dest, order, lengths):
    doc_ends = jnp.cumsum(lengths, axis=1).astype(jnp.int32)

    def one_sequence(seq_index):
        return sequence_attention(qkv, dest, order, doc_ends, seq_index)
    return lax.map(one_sequence, jnp.arange(PACKED_COUNT, dtype=jnp.int32))
```

```python
import functools
import math

import jax
import jax.numpy as jnp
from jax import lax
from jax.experimental import pallas as pl
from jax.experimental.pallas import tpu as pltpu
from jax.sharding import PartitionSpec as P

QUERY_HEADS = 32
KEY_VALUE_HEADS = 4
HEAD_SIZE = 128
QUERIES_PER_KV = 8
UNIT_HEADS = 4
PLACE_PARTS = 4
LAST_BATCHES = (4, 2, 1, 1)

MASK_FLOOR = -1e30
MESH = pl.DeviceIdType.MESH


def batches_of(units):
    return (units - sum(LAST_BATCHES), *LAST_BATCHES)


def batch_of(unit, starts):
    return sum(unit >= start for start in starts[1:])


def kernel(
    dp_count, ctx_count,
    qkv_ref, dest_hbm, order_hbm, lengths_hbm,
    out_ref,
    dest_ref, order_ref, lengths_ref, q_buf, kv_buf,
    early_bias, late_bias, settled_early_bias, settled_late_bias,
    own, arrived, moved_q, moved_kv, own_kv,
    local_sem, kv_send, kv_recv, out_send, out_recv, moved_send, moved_recv, corner_sem,
):
    dp_index = lax.axis_index("dp")
    me = lax.axis_index("ctx")
    above = lax.rem(dp_index + 1, dp_count)
    below = lax.rem(dp_index + dp_count - 1, dp_count)
    span = qkv_ref.shape[1]
    keys = ctx_count * span
    docs = lengths_ref.shape[1]
    query_width = QUERY_HEADS * HEAD_SIZE
    unit_cols = UNIT_HEADS * HEAD_SIZE
    moved = KEY_VALUE_HEADS - 1
    group_units = QUERIES_PER_KV // UNIT_HEADS
    units = moved * 2 * group_units
    batches = batches_of(units)
    starts = [sum(batches[:n]) for n in range(len(batches))]
    moved_first = moved * QUERIES_PER_KV * HEAD_SIZE
    moved_cols = pl.ds(moved_first, QUERIES_PER_KV * HEAD_SIZE)
    my_rows = pl.ds(pl.multiple_of(me * span, span), span)

    square = ctx_count == 4

    def target_of(k):
        if square:
            return (me + 1 - 2 * lax.rem(me, 2), lax.rem(me + 2, 4), 3 - me)[k - 1]
        return lax.rem(me + k, ctx_count)

    def origin_of(k):
        return target_of(k) if square else lax.rem(me + ctx_count - k, ctx_count)

    barrier = pltpu.get_barrier_semaphore()
    pl.semaphore_signal(barrier, inc=1, device_id={"dp": above}, device_id_type=MESH)
    pl.semaphore_signal(barrier, inc=1, device_id={"dp": below}, device_id_type=MESH)
    for k in range(1, 3 if square else ctx_count):
        pl.semaphore_signal(barrier, inc=1, device_id={"ctx": target_of(k)}, device_id_type=MESH)
    scalars = [
        pltpu.make_async_copy(source, target, sem)
        for source, target, sem in (
            (dest_hbm, dest_ref, out_send.at[0]),
            (order_hbm, order_ref, out_send.at[1]),
            (lengths_hbm, lengths_ref, local_sem.at[3]),
        )
    ]
    def load(first, width, target, sem):
        pltpu.make_async_copy(qkv_ref.at[:, :, pl.ds(first, width)], target, local_sem.at[sem]).start()

    def loaded(target, sem):
        pltpu.make_async_copy(target, target, local_sem.at[sem]).wait()

    def load_kv(g, target, sem):
        for part in range(2):
            first = query_width + (part * KEY_VALUE_HEADS + g) * HEAD_SIZE
            load(first, HEAD_SIZE, target.at[part], sem)

    later_kv = kv_buf.at[pl.ds(1, moved - 1), :, :, my_rows, :]
    load_kv(moved, own_kv, 0)
    load_kv(0, kv_buf.at[0, :, :, my_rows, :], 1)
    load(moved_first, query_width - moved_first, q_buf.at[:, :, moved_cols], 2)
    for copy in scalars:
        copy.start()

    pl.semaphore_wait(barrier, 4 if square else ctx_count + 1)
    if square:
        pl.semaphore_signal(corner_sem, inc=1, device_id={"ctx": target_of(1)}, device_id_type=MESH)

    first_late = KEY_VALUE_HEADS

    def block_of(index, rows):
        if index == 0:
            return kv_buf.at[0, :, 0, rows, :]
        if index == first_late:
            return kv_buf.at[0, :, 1, rows, :]
        return kv_buf.at[index, :, :, rows, :]

    def kv_copy(index, k):
        block = block_of(index, my_rows)
        return pltpu.make_async_remote_copy(
            src_ref=block, dst_ref=block, send_sem=kv_send, recv_sem=kv_recv.at[index],
            device_id={"ctx": target_of(k)}, device_id_type=MESH,
        )

    def others_of(index):
        return block_of(index, pl.ds(0, (ctx_count - 1) * span))

    def wait_bytes(ref, sem):
        pltpu.make_async_copy(ref, ref, sem).wait()

    def moved_copy(kind, up):
        return pltpu.make_async_remote_copy(
            src_ref=q_buf.at[:, :, moved_cols] if kind else own_kv,
            dst_ref=(moved_q if kind else moved_kv).at[up],
            send_sem=moved_send.at[kind],
            recv_sem=moved_recv.at[kind],
            device_id={"dp": above if up else below},
            device_id_type=MESH,
        )

    loaded(own_kv, 0)
    moved_copy(0, 1).start()
    moved_copy(0, 0).start()
    loaded(kv_buf.at[0, :, :, my_rows, :], 1)
    for k in range(1, ctx_count):
        if k == ctx_count - 1:
            loaded(q_buf.at[:, :, moved_cols], 2)
            moved_copy(1, 1).start()
            moved_copy(1, 0).start()
            if square:
                pl.semaphore_wait(corner_sem, 1)
        kv_copy(0, k).start()
    for k in range(1, ctx_count):
        kv_copy(first_late, k).start()

    first_cols = pl.ds(0, moved_first)
    load(0, moved_first, q_buf.at[:, :, first_cols], 2)
    for g in range(1, moved):
        load_kv(g, kv_buf.at[g, :, :, my_rows, :], 1)
    for copy in scalars:
        copy.wait()

    def ends_of(sequence):
        ends = []
        total_length = 0
        for d in range(docs):
            total_length = total_length + lengths_ref[sequence, d]
            ends.append(total_length)
        return ends

    own_ends = ends_of(dp_index)

    def identity_of(place, slots, settled):
        first = place < span
        position = jnp.where(
            first, order_ref[slots[0]] * span, order_ref[slots[1]] * span - span
        ) + place
        partners = dest_ref[0, slots[0]], dest_ref[0, slots[1]]
        counted = jnp.where(first, partners[0] * docs, partners[1] * docs)
        if settled:
            ends = [jnp.where(first, *pair) for pair in zip(ends_of(partners[0]), ends_of(partners[1]))]
        else:
            ends = own_ends
        for end in ends:
            counted = counted + (position >= end).astype(jnp.int32)
        return position, counted

    query_place = lax.broadcasted_iota(jnp.int32, (2 * span, 2 * span), 0)
    key_place = lax.broadcasted_iota(jnp.int32, (1, 2 * span), 1)

    def build_bias(settled, early_target, late_target):
        query_position, query_document = identity_of(query_place, (2 * me, 2 * me + 1), settled)
        for half in range(2):
            for b in range(0, ctx_count, 2):
                key_position, key_document = identity_of(
                    key_place, (2 * b + half, 2 * b + 2 + half), settled
                )
                visible = (key_document == query_document) & (key_position <= query_position)
                mask = jnp.where(visible, 0.0, MASK_FLOOR)
                if half == 0:
                    early_target[:, b * span:(b + 2) * span] = mask[:span]
                late_target[:, half * keys + b * span:half * keys + (b + 2) * span] = mask[span:]

    build_bias(False, early_bias, late_bias)
    loaded(later_kv, 1)
    for g in range(1, moved):
        for k in range(1, ctx_count):
            kv_copy(g, k).start()
    build_bias(True, settled_early_bias, settled_late_bias)
    loaded(q_buf.at[:, :, first_cols], 2)

    def settle_rows(half, kept, lower, upper):
        source = dest_ref[0, 2 * me + half]
        chosen = jnp.where(
            source == below, lower.astype(jnp.float32),
            jnp.where(source == above, upper.astype(jnp.float32), kept.astype(jnp.float32)),
        )
        return chosen.astype(jnp.bfloat16)

    def send(unit, batch):
        for up in range(2):
            pltpu.make_async_remote_copy(
                src_ref=own.at[unit],
                dst_ref=arrived.at[unit, up],
                send_sem=out_send.at[up],
                recv_sem=out_recv.at[batch],
                device_id={"dp": above if up else below},
                device_id_type=MESH,
            ).start()

    def send_one(unit):
        if isinstance(unit, int):
            send(unit, batch_of(unit, starts))
            return
        batch = sum((unit >= start).astype(jnp.int32) for start in starts[1:])
        send(unit, batch)

    exponent_scale = math.log2(math.e) / math.sqrt(HEAD_SIZE)

    def attend(queries, g, half, mask, between=None):
        width = keys * (1 + half)
        stacked = jnp.concatenate(queries, axis=0)
        key_rows, value_rows = (
            kv_buf[g, part].reshape(width, HEAD_SIZE) if half else kv_buf[g, part, 0]
            for part in range(2)
        )
        scores = lax.dot_general(
            stacked, key_rows, (((1,), (1,)), ((), ())), preferred_element_type=jnp.float32
        )
        if between is not None:
            between()
        scores = scores.reshape(len(queries), span, width) + mask[...][None]
        scores = scores.reshape(len(queries) * span, width)
        row_max = jnp.max(scores, axis=1, keepdims=True)
        weights = jnp.exp2((scores - row_max) * exponent_scale)
        total = jnp.sum(weights, axis=1, keepdims=True)
        mixed = jnp.dot(
            weights.astype(jnp.bfloat16), value_rows, preferred_element_type=jnp.float32
        )
        mixed = (mixed / total).astype(jnp.bfloat16)
        return [mixed[j * span:(j + 1) * span] for j in range(len(queries))]

    def head_cols(first, j):
        return pl.ds(pl.multiple_of(first + j * HEAD_SIZE, HEAD_SIZE), HEAD_SIZE)

    for g in range(moved):
        for half in range(2):
            if g == 0 or half == 0:
                index = first_late if g == 0 and half else g
                wait_bytes(others_of(index), kv_recv.at[index])

            def one_unit(i, carry):
                unit = (2 * g + half) * group_units + i
                first = (g * group_units + i) * unit_cols

                def send_last():
                    if g == 0 and half == 0:
                        @pl.when(i > 0)
                        def _():
                            send_one(unit - 1)
                    else:
                        send_one(unit - 1)

                heads = attend(
                    [q_buf[half, :, head_cols(first, j)] for j in range(UNIT_HEADS)],
                    g, half, late_bias if half else early_bias, send_last,
                )
                for j, head in enumerate(heads):
                    own[unit, :, j * HEAD_SIZE:(j + 1) * HEAD_SIZE] = head
                return carry

            if g == moved - 1 and half == 0:
                for k in range(1, ctx_count):
                    kv_copy(moved, k).start()
            lax.fori_loop(0, group_units, one_unit, 0)
        if g == max(moved - 2, 0):
            wait_bytes(moved_kv, moved_recv.at[0])
            for part in range(2):
                for half in range(2):
                    kv_buf[moved, part, half, my_rows, :] = settle_rows(
                        half, own_kv[part, half], moved_kv[1, part, half], moved_kv[0, part, half]
                    )
    send_one(units - 1)

    wait_bytes(moved_q, moved_recv.at[1])
    wait_bytes(others_of(moved), kv_recv.at[moved])

    for half in range(2):
        def one_moved(i, carry):
            queries = []
            for j in range(UNIT_HEADS):
                inner = head_cols(i * unit_cols, j)
                queries.append(settle_rows(
                    half, q_buf[half, :, head_cols(moved_first + i * unit_cols, j)],
                    moved_q[1, half, :, inner], moved_q[0, half, :, inner],
                ))
            heads = attend(queries, moved, half, settled_late_bias if half else settled_early_bias)
            for j, head in enumerate(heads):
                out_ref[half, :, head_cols(moved_first + i * unit_cols, j)] = head
            return carry

        lax.fori_loop(0, group_units, one_moved, 0)

    wait_bytes(moved_kv, moved_send.at[0])
    wait_bytes(moved_q, moved_send.at[1])
    wait_bytes(kv_buf.at[:, :, :, pl.ds(0, (ctx_count - 1) * span), :], kv_send)

    def settle(unit, carry):
        half = lax.rem(lax.div(unit, group_units), 2)
        first = (lax.div(unit, 2 * group_units) * group_units + lax.rem(unit, group_units)) * unit_cols
        for j in range(UNIT_HEADS):
            part = pl.ds(j * HEAD_SIZE, HEAD_SIZE)
            out_ref[half, :, head_cols(first, j)] = settle_rows(
                half, own[unit, :, part], arrived[unit, 1, :, part], arrived[unit, 0, :, part]
            )
        return carry

    for batch, (start, size) in enumerate(zip(starts, batches)):
        if batch == len(batches) - 1:
            for up in range(2):
                wait_bytes(own, out_send.at[up])
        wait_bytes(arrived.at[pl.ds(start, size)], out_recv.at[batch])
        lax.fori_loop(start, start + size, settle, 0)


def place_kernel(settled_ref, out_ref, sems):
    rows = settled_ref.shape[1] // (PLACE_PARTS // 2)
    copies = [
        pltpu.make_async_copy(
            settled_ref.at[half, pl.ds(i * rows, rows), :],
            out_ref.at[half, pl.ds(i * rows, rows), :],
            sems.at[half * (PLACE_PARTS // 2) + i],
        )
        for half in range(2) for i in range(PLACE_PARTS // 2)
    ]
    for copy in copies:
        copy.start()
    for copy in copies:
        copy.wait()


def on_device(dp_count, ctx_count, qkv, dest, order, lengths):
    span = qkv.shape[1] // 2
    query_width = QUERY_HEADS * HEAD_SIZE
    group_width = QUERIES_PER_KV * HEAD_SIZE
    units = 2 * (QUERY_HEADS - QUERIES_PER_KV) // UNIT_HEADS
    unit_shape = (units, span, UNIT_HEADS * HEAD_SIZE)
    keys = ctx_count * span
    qkv = qkv.reshape(2, span, qkv.shape[2])
    qkv, dest, order, lengths = (
        pltpu.with_memory_space_constraint(array, pltpu.HBM)
        for array in (qkv, dest, order, lengths)
    )
    settled = pl.pallas_call(
        functools.partial(kernel, dp_count, ctx_count),
        out_shape=pltpu.VMEM((2, span, query_width), jnp.bfloat16),
        in_specs=[pl.BlockSpec(memory_space=pltpu.HBM)] * 4,
        out_specs=pl.BlockSpec(memory_space=pltpu.VMEM),
        scratch_shapes=[
            pltpu.SMEM(dest.shape, jnp.int32),
            pltpu.SMEM(order.shape, jnp.int32),
            pltpu.SMEM(lengths.shape, jnp.int32),
            pltpu.VMEM((2, span, query_width), jnp.bfloat16),
            pltpu.VMEM((KEY_VALUE_HEADS, 2, 2, keys, HEAD_SIZE), jnp.bfloat16),
            pltpu.VMEM((span, keys), jnp.float32),
            pltpu.VMEM((span, 2 * keys), jnp.float32),
            pltpu.VMEM((span, keys), jnp.float32),
            pltpu.VMEM((span, 2 * keys), jnp.float32),
            pltpu.VMEM(unit_shape, jnp.bfloat16),
            pltpu.VMEM((units, 2, *unit_shape[1:]), jnp.bfloat16),
            pltpu.VMEM((2, 2, span, group_width), jnp.bfloat16),
            pltpu.VMEM((2, 2, 2, span, HEAD_SIZE), jnp.bfloat16),
            pltpu.VMEM((2, 2, span, HEAD_SIZE), jnp.bfloat16),
            pltpu.SemaphoreType.DMA((4,)),
            pltpu.SemaphoreType.DMA,
            pltpu.SemaphoreType.DMA((KEY_VALUE_HEADS + 1,)),
            pltpu.SemaphoreType.DMA((2,)),
            pltpu.SemaphoreType.DMA((len(batches_of(units)),)),
            pltpu.SemaphoreType.DMA((2,)),
            pltpu.SemaphoreType.DMA((2,)),
            pltpu.SemaphoreType.REGULAR,
        ],
        compiler_params=pltpu.CompilerParams(collective_id=0, has_side_effects=True,
            vmem_limit_bytes=40 << 20),
    )(qkv, dest, order, lengths)
    placed = pl.pallas_call(
        place_kernel,
        out_shape=jax.ShapeDtypeStruct((2, span, query_width), jnp.bfloat16),
        in_specs=[pl.BlockSpec(memory_space=pltpu.VMEM)],
        out_specs=pl.BlockSpec(memory_space=pltpu.HBM),
        scratch_shapes=[pltpu.SemaphoreType.DMA((PLACE_PARTS,))],
        compiler_params=pltpu.CompilerParams(vmem_limit_bytes=8 << 20),
    )(settled)
    return placed.reshape(1, 2 * span, query_width)


def solution(mesh):
    return jax.shard_map(
        functools.partial(on_device, mesh.shape["dp"], mesh.shape["ctx"]),
        mesh=mesh,
        in_specs=(P("dp", "ctx", None), P("dp", None), P(), P()),
        out_specs=P("dp", "ctx", None),
        check_vma=False,
    )
```

```python
import functools
import math

import jax
import jax.numpy as jnp
from jax import lax
from jax.experimental import pallas as pl
from jax.experimental.pallas import tpu as pltpu
from jax.sharding import PartitionSpec as P

QUERY_HEADS = 32
KEY_VALUE_HEADS = 4
HEAD_SIZE = 128
QUERIES_PER_KV = 8
UNIT_HEADS = 4
PLACE_PARTS = 4
LAST_BATCHES = (2, 2)

MASK_FLOOR = -1e30
MESH = pl.DeviceIdType.MESH


def batches_of(units):
    return (units - sum(LAST_BATCHES), *LAST_BATCHES)


def batch_of(unit, starts):
    return sum(unit >= start for start in starts[1:])


def kernel(
    dp_count, ctx_count,
    qkv_ref, dest_hbm, order_hbm, lengths_hbm,
    out_ref,
    dest_ref, order_ref, lengths_ref, q_buf, kv_buf,
    early_bias, late_bias, settled_early_bias, settled_late_bias,
    own, arrived, moved_q, moved_kv, own_kv,
    local_sem, kv_send, kv_recv, out_send, out_recv, moved_send, moved_recv, corner_sem,
):
    dp_index = lax.axis_index("dp")
    me = lax.axis_index("ctx")
    above = lax.rem(dp_index + 1, dp_count)
    below = lax.rem(dp_index + dp_count - 1, dp_count)
    span = qkv_ref.shape[1]
    keys = ctx_count * span
    docs = lengths_ref.shape[1]
    query_width = QUERY_HEADS * HEAD_SIZE
    unit_cols = UNIT_HEADS * HEAD_SIZE
    moved = KEY_VALUE_HEADS - 1
    group_units = QUERIES_PER_KV // UNIT_HEADS
    units = moved * 2 * group_units
    batches = batches_of(units)
    starts = [sum(batches[:n]) for n in range(len(batches))]
    moved_first = moved * QUERIES_PER_KV * HEAD_SIZE
    moved_cols = pl.ds(moved_first, QUERIES_PER_KV * HEAD_SIZE)
    my_rows = pl.ds(pl.multiple_of(me * span, span), span)

    square = ctx_count == 4

    def target_of(k):
        if square:
            return (me + 1 - 2 * lax.rem(me, 2), lax.rem(me + 2, 4), 3 - me)[k - 1]
        return lax.rem(me + k, ctx_count)

    def origin_of(k):
        return target_of(k) if square else lax.rem(me + ctx_count - k, ctx_count)

    barrier = pltpu.get_barrier_semaphore()
    pl.semaphore_signal(barrier, inc=1, device_id={"dp": above}, device_id_type=MESH)
    pl.semaphore_signal(barrier, inc=1, device_id={"dp": below}, device_id_type=MESH)
    for k in range(1, 3 if square else ctx_count):
        pl.semaphore_signal(barrier, inc=1, device_id={"ctx": target_of(k)}, device_id_type=MESH)
    scalars = [
        pltpu.make_async_copy(source, target, sem)
        for source, target, sem in (
            (dest_hbm, dest_ref, out_send.at[0]),
            (order_hbm, order_ref, out_send.at[1]),
            (lengths_hbm, lengths_ref, local_sem.at[3]),
        )
    ]
    def load(first, width, target, sem):
        pltpu.make_async_copy(qkv_ref.at[:, :, pl.ds(first, width)], target, local_sem.at[sem]).start()

    def loaded(target, sem):
        pltpu.make_async_copy(target, target, local_sem.at[sem]).wait()

    def load_kv(g, target, sem):
        for part in range(2):
            first = query_width + (part * KEY_VALUE_HEADS + g) * HEAD_SIZE
            load(first, HEAD_SIZE, target.at[part], sem)

    later_kv = kv_buf.at[pl.ds(1, moved - 1), :, :, my_rows, :]
    load_kv(moved, own_kv, 0)
    load_kv(0, kv_buf.at[0, :, :, my_rows, :], 1)
    load(moved_first, query_width - moved_first, q_buf.at[:, :, moved_cols], 2)
    for copy in scalars:
        copy.start()

    pl.semaphore_wait(barrier, 4 if square else ctx_count + 1)
    if square:
        pl.semaphore_signal(corner_sem, inc=1, device_id={"ctx": target_of(1)}, device_id_type=MESH)

    first_late = KEY_VALUE_HEADS

    def block_of(index, rows):
        if index == 0:
            return kv_buf.at[0, :, 0, rows, :]
        if index == first_late:
            return kv_buf.at[0, :, 1, rows, :]
        return kv_buf.at[index, :, :, rows, :]

    def kv_copy(index, k):
        block = block_of(index, my_rows)
        return pltpu.make_async_remote_copy(
            src_ref=block, dst_ref=block, send_sem=kv_send, recv_sem=kv_recv.at[index],
            device_id={"ctx": target_of(k)}, device_id_type=MESH,
        )

    def others_of(index):
        return block_of(index, pl.ds(0, (ctx_count - 1) * span))

    def wait_bytes(ref, sem):
        pltpu.make_async_copy(ref, ref, sem).wait()

    def moved_copy(kind, up):
        return pltpu.make_async_remote_copy(
            src_ref=q_buf.at[:, :, moved_cols] if kind else own_kv,
            dst_ref=(moved_q if kind else moved_kv).at[up],
            send_sem=moved_send.at[kind],
            recv_sem=moved_recv.at[kind],
            device_id={"dp": above if up else below},
            device_id_type=MESH,
        )

    loaded(own_kv, 0)
    moved_copy(0, 1).start()
    moved_copy(0, 0).start()
    loaded(kv_buf.at[0, :, :, my_rows, :], 1)
    for k in range(1, ctx_count):
        if k == ctx_count - 1:
            loaded(q_buf.at[:, :, moved_cols], 2)
            moved_copy(1, 1).start()
            moved_copy(1, 0).start()
            if square:
                pl.semaphore_wait(corner_sem, 1)
        kv_copy(0, k).start()
    for k in range(1, ctx_count):
        kv_copy(first_late, k).start()

    first_cols = pl.ds(0, moved_first)
    load(0, moved_first, q_buf.at[:, :, first_cols], 2)
    for g in range(1, moved):
        load_kv(g, kv_buf.at[g, :, :, my_rows, :], 1)
    for copy in scalars:
        copy.wait()

    def ends_of(sequence):
        ends = []
        total_length = 0
        for d in range(docs):
            total_length = total_length + lengths_ref[sequence, d]
            ends.append(total_length)
        return ends

    own_ends = ends_of(dp_index)

    def identity_of(place, slots, settled):
        first = place < span
        position = jnp.where(
            first, order_ref[slots[0]] * span, order_ref[slots[1]] * span - span
        ) + place
        partners = dest_ref[0, slots[0]], dest_ref[0, slots[1]]
        counted = jnp.where(first, partners[0] * docs, partners[1] * docs)
        if settled:
            ends = [jnp.where(first, *pair) for pair in zip(ends_of(partners[0]), ends_of(partners[1]))]
        else:
            ends = own_ends
        for end in ends:
            counted = counted + (position >= end).astype(jnp.int32)
        return position, counted

    query_place = lax.broadcasted_iota(jnp.int32, (2 * span, 2 * span), 0)
    key_place = lax.broadcasted_iota(jnp.int32, (1, 2 * span), 1)

    def build_bias(settled, early_target, late_target):
        query_position, query_document = identity_of(query_place, (2 * me, 2 * me + 1), settled)
        for half in range(2):
            for b in range(0, ctx_count, 2):
                key_position, key_document = identity_of(
                    key_place, (2 * b + half, 2 * b + 2 + half), settled
                )
                visible = (key_document == query_document) & (key_position <= query_position)
                mask = jnp.where(visible, 0.0, MASK_FLOOR)
                if half == 0:
                    early_target[:, b * span:(b + 2) * span] = mask[:span]
                late_target[:, half * keys + b * span:half * keys + (b + 2) * span] = mask[span:]

    build_bias(False, early_bias, late_bias)
    loaded(later_kv, 1)
    for g in range(1, moved):
        for k in range(1, ctx_count):
            kv_copy(g, k).start()
    build_bias(True, settled_early_bias, settled_late_bias)
    loaded(q_buf.at[:, :, first_cols], 2)

    def settle_rows(half, kept, lower, upper):
        source = dest_ref[0, 2 * me + half]
        chosen = jnp.where(
            source == below, lower.astype(jnp.float32),
            jnp.where(source == above, upper.astype(jnp.float32), kept.astype(jnp.float32)),
        )
        return chosen.astype(jnp.bfloat16)

    odd = lax.rem(dp_index, 2)
    closing = (dp_index == 0) | (dp_index == dp_count - 1)

    def send(start, count, part="all"):
        some = pl.ds(start, count)
        for up in range(2):
            copy = pltpu.make_async_remote_copy(
                src_ref=own.at[some],
                dst_ref=arrived.at[up, some],
                send_sem=out_send.at[up],
                recv_sem=out_recv.at[batch_of(start, starts)],
                device_id={"dp": above if up else below},
                device_id_type=MESH,
            )
            if part == "all":
                copy.start()
            elif part == "prompt":
                pl.when((odd != up) | closing)(copy.start)
            else:
                pl.when((odd == up) & jnp.logical_not(closing))(copy.start)

    exponent_scale = math.log2(math.e) / math.sqrt(HEAD_SIZE)

    def attend(queries, g, half, mask, between=None):
        width = keys * (1 + half)
        stacked = jnp.concatenate(queries, axis=0)
        key_rows, value_rows = (
            kv_buf[g, part].reshape(width, HEAD_SIZE) if half else kv_buf[g, part, 0]
            for part in range(2)
        )
        scores = lax.dot_general(
            stacked, key_rows, (((1,), (1,)), ((), ())), preferred_element_type=jnp.float32
        )
        if between is not None:
            between()
        scores = scores.reshape(len(queries), span, width) + mask[...][None]
        scores = scores.reshape(len(queries) * span, width)
        row_max = jnp.max(scores, axis=1, keepdims=True)
        weights = jnp.exp2((scores - row_max) * exponent_scale)
        total = jnp.sum(weights, axis=1, keepdims=True)
        mixed = jnp.dot(
            weights.astype(jnp.bfloat16), value_rows, preferred_element_type=jnp.float32
        )
        mixed = (mixed / total).astype(jnp.bfloat16)
        return [mixed[j * span:(j + 1) * span] for j in range(len(queries))]

    def head_cols(first, j):
        return pl.ds(pl.multiple_of(first + j * HEAD_SIZE, HEAD_SIZE), HEAD_SIZE)

    for g in range(moved):
        for half in range(2):
            if g == 0 or half == 0:
                index = first_late if g == 0 and half else g
                wait_bytes(others_of(index), kv_recv.at[index])

            phase = 2 * g + half
            before = phase * group_units

            def one_unit(i, carry):
                unit = before + i
                first = (g * group_units + i) * unit_cols

                def send_done():
                    if g > 0:
                        if phase > 2:
                            pl.when(i == 0)(lambda: send(before - group_units, group_units))
                        return
                    for n in range(group_units):
                        if before + n > 0:
                            pl.when(i == n)(lambda: send(before + n - 1, 1, "prompt"))

                heads = attend(
                    [q_buf[half, :, head_cols(first, j)] for j in range(UNIT_HEADS)],
                    g, half, late_bias if half else early_bias, send_done,
                )
                for j, head in enumerate(heads):
                    own[unit, :, j * HEAD_SIZE:(j + 1) * HEAD_SIZE] = head
                return carry

            if g == moved - 1 and half == 0:
                for k in range(1, ctx_count):
                    kv_copy(moved, k).start()
            lax.fori_loop(0, group_units, one_unit, 0)
            if phase == 1:
                send(before + group_units - 1, 1, "prompt")
                send(0, before + group_units, "held")
        if g == max(moved - 2, 0):
            wait_bytes(moved_kv, moved_recv.at[0])
            for part in range(2):
                for half in range(2):
                    kv_buf[moved, part, half, my_rows, :] = settle_rows(
                        half, own_kv[part, half], moved_kv[1, part, half], moved_kv[0, part, half]
                    )
    send(units - group_units, group_units)

    wait_bytes(moved_q, moved_recv.at[1])
    wait_bytes(others_of(moved), kv_recv.at[moved])

    for half in range(2):
        def one_moved(i, carry):
            queries = []
            for j in range(UNIT_HEADS):
                inner = head_cols(i * unit_cols, j)
                queries.append(settle_rows(
                    half, q_buf[half, :, head_cols(moved_first + i * unit_cols, j)],
                    moved_q[1, half, :, inner], moved_q[0, half, :, inner],
                ))
            heads = attend(queries, moved, half, settled_late_bias if half else settled_early_bias)
            for j, head in enumerate(heads):
                out_ref[half, :, head_cols(moved_first + i * unit_cols, j)] = head
            return carry

        lax.fori_loop(0, group_units, one_moved, 0)

    wait_bytes(moved_kv, moved_send.at[0])
    wait_bytes(moved_q, moved_send.at[1])
    wait_bytes(kv_buf.at[:, :, :, pl.ds(0, (ctx_count - 1) * span), :], kv_send)

    def settle(unit, carry):
        half = lax.rem(lax.div(unit, group_units), 2)
        first = (lax.div(unit, 2 * group_units) * group_units + lax.rem(unit, group_units)) * unit_cols
        for j in range(UNIT_HEADS):
            part = pl.ds(j * HEAD_SIZE, HEAD_SIZE)
            out_ref[half, :, head_cols(first, j)] = settle_rows(
                half, own[unit, :, part], arrived[1, unit, :, part], arrived[0, unit, :, part]
            )
        return carry

    for batch, (start, size) in enumerate(zip(starts, batches)):
        if batch == len(batches) - 1:
            for up in range(2):
                wait_bytes(own, out_send.at[up])
        wait_bytes(arrived.at[:, pl.ds(start, size)], out_recv.at[batch])
        lax.fori_loop(start, start + size, settle, 0)


def place_kernel(settled_ref, out_ref, sem):
    rows = settled_ref.shape[1] // (PLACE_PARTS // 2)
    copies = [
        pltpu.make_async_copy(
            settled_ref.at[half, pl.ds(i * rows, rows), :],
            out_ref.at[half, pl.ds(i * rows, rows), :],
            sem,
        )
        for half in range(2) for i in range(PLACE_PARTS // 2)
    ]
    for copy in copies:
        copy.start()
    pltpu.make_async_copy(settled_ref, out_ref, sem).wait()


def on_device(dp_count, ctx_count, qkv, dest, order, lengths):
    span = qkv.shape[1] // 2
    query_width = QUERY_HEADS * HEAD_SIZE
    group_width = QUERIES_PER_KV * HEAD_SIZE
    units = 2 * (QUERY_HEADS - QUERIES_PER_KV) // UNIT_HEADS
    unit_shape = (units, span, UNIT_HEADS * HEAD_SIZE)
    keys = ctx_count * span
    qkv = qkv.reshape(2, span, qkv.shape[2])
    qkv, dest, order, lengths = (
        pltpu.with_memory_space_constraint(array, pltpu.HBM)
        for array in (qkv, dest, order, lengths)
    )
    settled = pl.pallas_call(
        functools.partial(kernel, dp_count, ctx_count),
        out_shape=pltpu.VMEM((2, span, query_width), jnp.bfloat16),
        in_specs=[pl.BlockSpec(memory_space=pltpu.HBM)] * 4,
        out_specs=pl.BlockSpec(memory_space=pltpu.VMEM),
        scratch_shapes=[
            pltpu.SMEM(dest.shape, jnp.int32),
            pltpu.SMEM(order.shape, jnp.int32),
            pltpu.SMEM(lengths.shape, jnp.int32),
            pltpu.VMEM((2, span, query_width), jnp.bfloat16),
            pltpu.VMEM((KEY_VALUE_HEADS, 2, 2, keys, HEAD_SIZE), jnp.bfloat16),
            pltpu.VMEM((span, keys), jnp.float32),
            pltpu.VMEM((span, 2 * keys), jnp.float32),
            pltpu.VMEM((span, keys), jnp.float32),
            pltpu.VMEM((span, 2 * keys), jnp.float32),
            pltpu.VMEM(unit_shape, jnp.bfloat16),
            pltpu.VMEM((2, *unit_shape), jnp.bfloat16),
            pltpu.VMEM((2, 2, span, group_width), jnp.bfloat16),
            pltpu.VMEM((2, 2, 2, span, HEAD_SIZE), jnp.bfloat16),
            pltpu.VMEM((2, 2, span, HEAD_SIZE), jnp.bfloat16),
            pltpu.SemaphoreType.DMA((4,)),
            pltpu.SemaphoreType.DMA,
            pltpu.SemaphoreType.DMA((KEY_VALUE_HEADS + 1,)),
            pltpu.SemaphoreType.DMA((2,)),
            pltpu.SemaphoreType.DMA((len(batches_of(units)),)),
            pltpu.SemaphoreType.DMA((2,)),
            pltpu.SemaphoreType.DMA((2,)),
            pltpu.SemaphoreType.REGULAR,
        ],
        compiler_params=pltpu.CompilerParams(collective_id=0, has_side_effects=True,
            vmem_limit_bytes=40 << 20),
    )(qkv, dest, order, lengths)
    placed = pl.pallas_call(
        place_kernel,
        out_shape=jax.ShapeDtypeStruct((2, span, query_width), jnp.bfloat16),
        in_specs=[pl.BlockSpec(memory_space=pltpu.VMEM)],
        out_specs=pl.BlockSpec(memory_space=pltpu.HBM),
        scratch_shapes=[pltpu.SemaphoreType.DMA],
        compiler_params=pltpu.CompilerParams(vmem_limit_bytes=8 << 20),
    )(settled)
    return placed.reshape(1, 2 * span, query_width)


def solution(mesh):
    return jax.shard_map(
        functools.partial(on_device, mesh.shape["dp"], mesh.shape["ctx"]),
        mesh=mesh,
        in_specs=(P("dp", "ctx", None), P("dp", None), P(), P()),
        out_specs=P("dp", "ctx", None),
        check_vma=False,
    )
```

```python
import functools
import math

import jax
import jax.numpy as jnp
from jax import lax
from jax.experimental import pallas as pl
from jax.experimental.pallas import tpu as pltpu
from jax.sharding import PartitionSpec as P

QUERY_HEADS = 32
KEY_VALUE_HEADS = 4
HEAD_SIZE = 128
QUERIES_PER_KV = 8
UNIT_HEADS = 4
PLACE_PARTS = 4
LAST_BATCHES = (2,)

MASK_FLOOR = -1e30
MESH = pl.DeviceIdType.MESH


def batches_of(units):
    return (units - sum(LAST_BATCHES), *LAST_BATCHES)


def batch_of(unit, starts):
    return sum(unit >= start for start in starts[1:])


def kernel(
    dp_count, ctx_count,
    qkv_ref, dest_hbm, order_hbm, lengths_hbm,
    out_ref,
    dest_ref, order_ref, lengths_ref, q_buf, kv_buf,
    early_bias, late_bias, settled_early_bias, settled_late_bias,
    own, arrived, moved_q, moved_kv, own_kv,
    local_sem, kv_send, kv_recv, out_send, out_recv, moved_send, moved_recv, corner_sem,
):
    dp_index = lax.axis_index("dp")
    me = lax.axis_index("ctx")
    above = lax.rem(dp_index + 1, dp_count)
    below = lax.rem(dp_index + dp_count - 1, dp_count)
    span = qkv_ref.shape[1]
    keys = ctx_count * span
    docs = lengths_ref.shape[1]
    query_width = QUERY_HEADS * HEAD_SIZE
    unit_cols = UNIT_HEADS * HEAD_SIZE
    moved = KEY_VALUE_HEADS - 1
    group_units = QUERIES_PER_KV // UNIT_HEADS
    units = moved * 2 * group_units
    batches = batches_of(units)
    starts = [sum(batches[:n]) for n in range(len(batches))]
    moved_first = moved * QUERIES_PER_KV * HEAD_SIZE
    moved_cols = pl.ds(moved_first, QUERIES_PER_KV * HEAD_SIZE)
    my_rows = pl.ds(pl.multiple_of(me * span, span), span)

    square = ctx_count == 4

    def target_of(k):
        if square:
            return (me + 1 - 2 * lax.rem(me, 2), lax.rem(me + 2, 4), 3 - me)[k - 1]
        return lax.rem(me + k, ctx_count)

    def origin_of(k):
        return target_of(k) if square else lax.rem(me + ctx_count - k, ctx_count)

    barrier = pltpu.get_barrier_semaphore()
    pl.semaphore_signal(barrier, inc=1, device_id={"dp": above}, device_id_type=MESH)
    pl.semaphore_signal(barrier, inc=1, device_id={"dp": below}, device_id_type=MESH)
    for k in range(1, 3 if square else ctx_count):
        pl.semaphore_signal(barrier, inc=1, device_id={"ctx": target_of(k)}, device_id_type=MESH)
    scalars = [
        pltpu.make_async_copy(source, target, sem)
        for source, target, sem in (
            (dest_hbm, dest_ref, out_send.at[0]),
            (order_hbm, order_ref, out_send.at[1]),
            (lengths_hbm, lengths_ref, local_sem.at[3]),
        )
    ]
    def load(first, width, target, sem):
        pltpu.make_async_copy(qkv_ref.at[:, :, pl.ds(first, width)], target, local_sem.at[sem]).start()

    def loaded(target, sem):
        pltpu.make_async_copy(target, target, local_sem.at[sem]).wait()

    def load_kv(g, target, sem):
        for part in range(2):
            first = query_width + (part * KEY_VALUE_HEADS + g) * HEAD_SIZE
            load(first, HEAD_SIZE, target.at[part], sem)

    later_kv = kv_buf.at[pl.ds(1, moved - 1), :, :, my_rows, :]
    load_kv(moved, own_kv, 0)
    load_kv(0, kv_buf.at[0, :, :, my_rows, :], 1)
    load(moved_first, query_width - moved_first, q_buf.at[:, :, moved_cols], 2)
    for copy in scalars:
        copy.start()

    pl.semaphore_wait(barrier, 4 if square else ctx_count + 1)
    if square:
        pl.semaphore_signal(corner_sem, inc=1, device_id={"ctx": target_of(1)}, device_id_type=MESH)

    first_late = KEY_VALUE_HEADS

    def block_of(index, rows):
        if index == 0:
            return kv_buf.at[0, :, 0, rows, :]
        if index == first_late:
            return kv_buf.at[0, :, 1, rows, :]
        return kv_buf.at[index, :, :, rows, :]

    def kv_copy(index, k):
        block = block_of(index, my_rows)
        return pltpu.make_async_remote_copy(
            src_ref=block, dst_ref=block, send_sem=kv_send, recv_sem=kv_recv.at[index],
            device_id={"ctx": target_of(k)}, device_id_type=MESH,
        )

    def others_of(index):
        return block_of(index, pl.ds(0, (ctx_count - 1) * span))

    def wait_bytes(ref, sem):
        pltpu.make_async_copy(ref, ref, sem).wait()

    def moved_copy(kind, up):
        return pltpu.make_async_remote_copy(
            src_ref=q_buf.at[:, :, moved_cols] if kind else own_kv,
            dst_ref=(moved_q if kind else moved_kv).at[up],
            send_sem=moved_send.at[kind],
            recv_sem=moved_recv.at[kind],
            device_id={"dp": above if up else below},
            device_id_type=MESH,
        )

    loaded(own_kv, 0)
    moved_copy(0, 1).start()
    moved_copy(0, 0).start()
    loaded(kv_buf.at[0, :, :, my_rows, :], 1)
    for k in range(1, ctx_count):
        if k == ctx_count - 1:
            loaded(q_buf.at[:, :, moved_cols], 2)
            moved_copy(1, 1).start()
            moved_copy(1, 0).start()
            if square:
                pl.semaphore_wait(corner_sem, 1)
        kv_copy(0, k).start()
    for k in range(1, ctx_count):
        kv_copy(first_late, k).start()

    first_cols = pl.ds(0, moved_first)
    load(0, moved_first, q_buf.at[:, :, first_cols], 2)
    for g in range(1, moved):
        load_kv(g, kv_buf.at[g, :, :, my_rows, :], 1)
    for copy in scalars:
        copy.wait()

    def ends_of(sequence):
        ends = []
        total_length = 0
        for d in range(docs):
            total_length = total_length + lengths_ref[sequence, d]
            ends.append(total_length)
        return ends

    own_ends = ends_of(dp_index)

    def identity_of(place, slots, settled):
        first = place < span
        position = jnp.where(
            first, order_ref[slots[0]] * span, order_ref[slots[1]] * span - span
        ) + place
        partners = dest_ref[0, slots[0]], dest_ref[0, slots[1]]
        counted = jnp.where(first, partners[0] * docs, partners[1] * docs)
        if settled:
            ends = [jnp.where(first, *pair) for pair in zip(ends_of(partners[0]), ends_of(partners[1]))]
        else:
            ends = own_ends
        for end in ends:
            counted = counted + (position >= end).astype(jnp.int32)
        return position, counted

    query_place = lax.broadcasted_iota(jnp.int32, (2 * span, 2 * span), 0)
    key_place = lax.broadcasted_iota(jnp.int32, (1, 2 * span), 1)

    def build_bias(settled, early_target, late_target):
        query_position, query_document = identity_of(query_place, (2 * me, 2 * me + 1), settled)
        for half in range(2):
            for b in range(0, ctx_count, 2):
                key_position, key_document = identity_of(
                    key_place, (2 * b + half, 2 * b + 2 + half), settled
                )
                visible = (key_document == query_document) & (key_position <= query_position)
                mask = jnp.where(visible, 0.0, MASK_FLOOR)
                if half == 0:
                    early_target[:, b * span:(b + 2) * span] = mask[:span]
                late_target[:, half * keys + b * span:half * keys + (b + 2) * span] = mask[span:]

    build_bias(False, early_bias, late_bias)
    loaded(later_kv, 1)
    for g in range(1, moved):
        for k in range(1, ctx_count):
            kv_copy(g, k).start()
    build_bias(True, settled_early_bias, settled_late_bias)
    loaded(q_buf.at[:, :, first_cols], 2)

    def settle_rows(half, kept, lower, upper):
        source = dest_ref[0, 2 * me + half]
        chosen = jnp.where(
            source == below, lower.astype(jnp.float32),
            jnp.where(source == above, upper.astype(jnp.float32), kept.astype(jnp.float32)),
        )
        return chosen.astype(jnp.bfloat16)

    odd = lax.rem(dp_index, 2)
    closing = (dp_index == 0) | (dp_index == dp_count - 1)
    links_before = lax.div(jnp.where(odd == 1, dp_index, dp_count - 2 - dp_index), 2)
    holds = jnp.logical_not(closing) & (links_before < dp_count // 2 - 2)

    def send(start, count, part="all"):
        some = pl.ds(start, count)
        for up in range(2):
            copy = pltpu.make_async_remote_copy(
                src_ref=own.at[some],
                dst_ref=arrived.at[up, some],
                send_sem=out_send.at[up],
                recv_sem=out_recv.at[batch_of(start, starts)],
                device_id={"dp": above if up else below},
                device_id_type=MESH,
            )
            if part == "all":
                copy.start()
            else:
                held = (odd == up) & holds
                pl.when(held if part == "held" else jnp.logical_not(held))(copy.start)

    exponent_scale = math.log2(math.e) / math.sqrt(HEAD_SIZE)

    def attend(queries, g, half, mask, between=None):
        width = keys * (1 + half)
        stacked = jnp.concatenate(queries, axis=0)
        key_rows, value_rows = (
            kv_buf[g, part].reshape(width, HEAD_SIZE) if half else kv_buf[g, part, 0]
            for part in range(2)
        )
        scores = lax.dot_general(
            stacked, key_rows, (((1,), (1,)), ((), ())), preferred_element_type=jnp.float32
        )
        if between is not None:
            between()
        scores = scores.reshape(len(queries), span, width) + mask[...][None]
        scores = scores.reshape(len(queries) * span, width)
        row_max = jnp.max(scores, axis=1, keepdims=True)
        weights = jnp.exp2((scores - row_max) * exponent_scale)
        total = jnp.sum(weights, axis=1, keepdims=True)
        mixed = jnp.dot(
            weights.astype(jnp.bfloat16), value_rows, preferred_element_type=jnp.float32
        )
        mixed = (mixed / total).astype(jnp.bfloat16)
        return [mixed[j * span:(j + 1) * span] for j in range(len(queries))]

    def head_cols(first, j):
        return pl.ds(pl.multiple_of(first + j * HEAD_SIZE, HEAD_SIZE), HEAD_SIZE)

    for g in range(moved):
        for half in range(2):
            if g == 0 or half == 0:
                index = first_late if g == 0 and half else g
                wait_bytes(others_of(index), kv_recv.at[index])

            phase = 2 * g + half
            before = phase * group_units

            def one_unit(i, carry):
                unit = before + i
                first = (g * group_units + i) * unit_cols

                def send_done():
                    if g > 0:
                        if phase > 2:
                            pl.when(i == 0)(lambda: send(before - group_units, group_units))
                        return
                    for n in range(group_units):
                        if before + n > 0:
                            pl.when(i == n)(lambda: send(before + n - 1, 1, "prompt"))

                heads = attend(
                    [q_buf[half, :, head_cols(first, j)] for j in range(UNIT_HEADS)],
                    g, half, late_bias if half else early_bias, send_done,
                )
                for j, head in enumerate(heads):
                    own[unit, :, j * HEAD_SIZE:(j + 1) * HEAD_SIZE] = head
                return carry

            if g == moved - 1 and half == 0:
                for k in range(1, ctx_count):
                    kv_copy(moved, k).start()
            lax.fori_loop(0, group_units, one_unit, 0)
            if phase == 1:
                send(before + group_units - 1, 1, "prompt")
                send(0, before + group_units, "held")
        if g == max(moved - 2, 0):
            wait_bytes(moved_kv, moved_recv.at[0])
            for part in range(2):
                for half in range(2):
                    kv_buf[moved, part, half, my_rows, :] = settle_rows(
                        half, own_kv[part, half], moved_kv[1, part, half], moved_kv[0, part, half]
                    )
    send(units - group_units, group_units)

    wait_bytes(moved_q, moved_recv.at[1])
    wait_bytes(others_of(moved), kv_recv.at[moved])

    for half in range(2):
        def one_moved(i, carry):
            queries = []
            for j in range(UNIT_HEADS):
                inner = head_cols(i * unit_cols, j)
                queries.append(settle_rows(
                    half, q_buf[half, :, head_cols(moved_first + i * unit_cols, j)],
                    moved_q[1, half, :, inner], moved_q[0, half, :, inner],
                ))
            heads = attend(queries, moved, half, settled_late_bias if half else settled_early_bias)
            for j, head in enumerate(heads):
                out_ref[half, :, head_cols(moved_first + i * unit_cols, j)] = head
            return carry

        lax.fori_loop(0, group_units, one_moved, 0)

    wait_bytes(moved_kv, moved_send.at[0])
    wait_bytes(moved_q, moved_send.at[1])
    wait_bytes(kv_buf.at[:, :, :, pl.ds(0, (ctx_count - 1) * span), :], kv_send)

    def settle(unit, carry):
        half = lax.rem(lax.div(unit, group_units), 2)
        first = (lax.div(unit, 2 * group_units) * group_units + lax.rem(unit, group_units)) * unit_cols
        for j in range(UNIT_HEADS):
            part = pl.ds(j * HEAD_SIZE, HEAD_SIZE)
            out_ref[half, :, head_cols(first, j)] = settle_rows(
                half, own[unit, :, part], arrived[1, unit, :, part], arrived[0, unit, :, part]
            )
        return carry

    for batch, (start, size) in enumerate(zip(starts, batches)):
        if batch == len(batches) - 1:
            for up in range(2):
                wait_bytes(own, out_send.at[up])
        wait_bytes(arrived.at[:, pl.ds(start, size)], out_recv.at[batch])
        lax.fori_loop(start, start + size, settle, 0)


def place_kernel(settled_ref, out_ref, sem):
    rows = settled_ref.shape[1] // (PLACE_PARTS // 2)
    copies = [
        pltpu.make_async_copy(
            settled_ref.at[half, pl.ds(i * rows, rows), :],
            out_ref.at[half, pl.ds(i * rows, rows), :],
            sem,
        )
        for half in range(2) for i in range(PLACE_PARTS // 2)
    ]
    for copy in copies:
        copy.start()
    pltpu.make_async_copy(settled_ref, out_ref, sem).wait()


def on_device(dp_count, ctx_count, qkv, dest, order, lengths):
    span = qkv.shape[1] // 2
    query_width = QUERY_HEADS * HEAD_SIZE
    group_width = QUERIES_PER_KV * HEAD_SIZE
    units = 2 * (QUERY_HEADS - QUERIES_PER_KV) // UNIT_HEADS
    unit_shape = (units, span, UNIT_HEADS * HEAD_SIZE)
    keys = ctx_count * span
    qkv = qkv.reshape(2, span, qkv.shape[2])
    qkv, dest, order, lengths = (
        pltpu.with_memory_space_constraint(array, pltpu.HBM)
        for array in (qkv, dest, order, lengths)
    )
    settled = pl.pallas_call(
        functools.partial(kernel, dp_count, ctx_count),
        out_shape=pltpu.VMEM((2, span, query_width), jnp.bfloat16),
        in_specs=[pl.BlockSpec(memory_space=pltpu.HBM)] * 4,
        out_specs=pl.BlockSpec(memory_space=pltpu.VMEM),
        scratch_shapes=[
            pltpu.SMEM(dest.shape, jnp.int32),
            pltpu.SMEM(order.shape, jnp.int32),
            pltpu.SMEM(lengths.shape, jnp.int32),
            pltpu.VMEM((2, span, query_width), jnp.bfloat16),
            pltpu.VMEM((KEY_VALUE_HEADS, 2, 2, keys, HEAD_SIZE), jnp.bfloat16),
            pltpu.VMEM((span, keys), jnp.float32),
            pltpu.VMEM((span, 2 * keys), jnp.float32),
            pltpu.VMEM((span, keys), jnp.float32),
            pltpu.VMEM((span, 2 * keys), jnp.float32),
            pltpu.VMEM(unit_shape, jnp.bfloat16),
            pltpu.VMEM((2, *unit_shape), jnp.bfloat16),
            pltpu.VMEM((2, 2, span, group_width), jnp.bfloat16),
            pltpu.VMEM((2, 2, 2, span, HEAD_SIZE), jnp.bfloat16),
            pltpu.VMEM((2, 2, span, HEAD_SIZE), jnp.bfloat16),
            pltpu.SemaphoreType.DMA((4,)),
            pltpu.SemaphoreType.DMA,
            pltpu.SemaphoreType.DMA((KEY_VALUE_HEADS + 1,)),
            pltpu.SemaphoreType.DMA((2,)),
            pltpu.SemaphoreType.DMA((len(batches_of(units)),)),
            pltpu.SemaphoreType.DMA((2,)),
            pltpu.SemaphoreType.DMA((2,)),
            pltpu.SemaphoreType.REGULAR,
        ],
        compiler_params=pltpu.CompilerParams(collective_id=0, has_side_effects=True,
            vmem_limit_bytes=40 << 20),
    )(qkv, dest, order, lengths)
    placed = pl.pallas_call(
        place_kernel,
        out_shape=jax.ShapeDtypeStruct((2, span, query_width), jnp.bfloat16),
        in_specs=[pl.BlockSpec(memory_space=pltpu.VMEM)],
        out_specs=pl.BlockSpec(memory_space=pltpu.HBM),
        scratch_shapes=[pltpu.SemaphoreType.DMA],
        compiler_params=pltpu.CompilerParams(vmem_limit_bytes=8 << 20),
    )(settled)
    return placed.reshape(1, 2 * span, query_width)


def solution(mesh):
    return jax.shard_map(
        functools.partial(on_device, mesh.shape["dp"], mesh.shape["ctx"]),
        mesh=mesh,
        in_specs=(P("dp", "ctx", None), P("dp", None), P(), P()),
        out_specs=P("dp", "ctx", None),
        check_vma=False,
    )
```

```python
import functools
import math

import jax
import jax.numpy as jnp
from jax import lax
from jax.experimental import pallas as pl
from jax.experimental.pallas import tpu as pltpu
from jax.sharding import PartitionSpec as P

QUERY_HEADS = 32
KEY_VALUE_HEADS = 4
HEAD_SIZE = 128
QUERIES_PER_KV = 8
UNIT_HEADS = 4
PLACE_PARTS = 4
LAST_BATCHES = (2,)

MASK_FLOOR = -1e30
MESH = pl.DeviceIdType.MESH


def batches_of(units):
    return (units - sum(LAST_BATCHES), *LAST_BATCHES)


def batch_of(unit, starts):
    return sum(unit >= start for start in starts[1:])


def kernel(
    dp_count, ctx_count,
    qkv_ref, dest_hbm, order_hbm, lengths_hbm,
    out_ref,
    dest_ref, order_ref, lengths_ref, q_buf, kv_buf,
    early_bias, late_bias, settled_early_bias, settled_late_bias,
    own, arrived, moved_q, moved_kv, own_kv,
    local_sem, kv_send, kv_recv, out_send, out_recv, moved_send, moved_recv, corner_sem,
):
    dp_index = lax.axis_index("dp")
    me = lax.axis_index("ctx")
    above = lax.rem(dp_index + 1, dp_count)
    below = lax.rem(dp_index + dp_count - 1, dp_count)
    span = qkv_ref.shape[1]
    keys = ctx_count * span
    docs = lengths_ref.shape[1]
    query_width = QUERY_HEADS * HEAD_SIZE
    unit_cols = UNIT_HEADS * HEAD_SIZE
    moved = KEY_VALUE_HEADS - 1
    group_units = QUERIES_PER_KV // UNIT_HEADS
    units = moved * 2 * group_units
    batches = batches_of(units)
    starts = [sum(batches[:n]) for n in range(len(batches))]
    moved_first = moved * QUERIES_PER_KV * HEAD_SIZE
    moved_cols = pl.ds(moved_first, QUERIES_PER_KV * HEAD_SIZE)
    my_rows = pl.ds(pl.multiple_of(me * span, span), span)

    square = ctx_count == 4

    def target_of(k):
        if square:
            return (me + 1 - 2 * lax.rem(me, 2), lax.rem(me + 2, 4), 3 - me)[k - 1]
        return lax.rem(me + k, ctx_count)

    def origin_of(k):
        return target_of(k) if square else lax.rem(me + ctx_count - k, ctx_count)

    barrier = pltpu.get_barrier_semaphore()
    pl.semaphore_signal(barrier, inc=1, device_id={"dp": above}, device_id_type=MESH)
    pl.semaphore_signal(barrier, inc=1, device_id={"dp": below}, device_id_type=MESH)
    for k in range(1, 3 if square else ctx_count):
        pl.semaphore_signal(barrier, inc=1, device_id={"ctx": target_of(k)}, device_id_type=MESH)
    scalars = [
        pltpu.make_async_copy(source, target, sem)
        for source, target, sem in (
            (dest_hbm, dest_ref, out_send.at[0]),
            (order_hbm, order_ref, out_send.at[1]),
            (lengths_hbm, lengths_ref, local_sem.at[2]),
        )
    ]
    def load(first, width, target, sem):
        pltpu.make_async_copy(qkv_ref.at[:, :, pl.ds(first, width)], target, sem).start()

    def loaded(target, sem):
        pltpu.make_async_copy(target, target, sem).wait()

    def load_kv(g, target, sem):
        for part in range(2):
            first = query_width + (part * KEY_VALUE_HEADS + g) * HEAD_SIZE
            load(first, HEAD_SIZE, target.at[part], sem)

    later_kv = kv_buf.at[pl.ds(1, moved - 1), :, :, my_rows, :]
    load_kv(moved, own_kv, kv_send)
    load_kv(0, kv_buf.at[0, :, :, my_rows, :], local_sem.at[0])
    load(moved_first, query_width - moved_first, q_buf.at[:, :, moved_cols], local_sem.at[1])
    for copy in scalars:
        copy.start()

    pl.semaphore_wait(barrier, 4 if square else ctx_count + 1)
    if square:
        pl.semaphore_signal(corner_sem, inc=1, device_id={"ctx": target_of(1)}, device_id_type=MESH)

    first_late = KEY_VALUE_HEADS

    def block_of(index, rows):
        if index == 0:
            return kv_buf.at[0, :, 0, rows, :]
        if index == first_late:
            return kv_buf.at[0, :, 1, rows, :]
        return kv_buf.at[index, :, :, rows, :]

    def kv_copy(index, k):
        block = block_of(index, my_rows)
        return pltpu.make_async_remote_copy(
            src_ref=block, dst_ref=block, send_sem=kv_send, recv_sem=kv_recv.at[index],
            device_id={"ctx": target_of(k)}, device_id_type=MESH,
        )

    def others_of(index):
        return block_of(index, pl.ds(0, (ctx_count - 1) * span))

    def wait_bytes(ref, sem):
        pltpu.make_async_copy(ref, ref, sem).wait()

    def moved_copy(kind, up):
        return pltpu.make_async_remote_copy(
            src_ref=q_buf.at[:, :, moved_cols] if kind else own_kv,
            dst_ref=(moved_q if kind else moved_kv).at[up],
            send_sem=moved_send,
            recv_sem=moved_recv.at[kind],
            device_id={"dp": above if up else below},
            device_id_type=MESH,
        )

    loaded(own_kv, kv_send)
    moved_copy(0, 1).start()
    moved_copy(0, 0).start()
    loaded(kv_buf.at[0, :, :, my_rows, :], local_sem.at[0])
    for k in range(1, ctx_count):
        if k == ctx_count - 1:
            loaded(q_buf.at[:, :, moved_cols], local_sem.at[1])
            moved_copy(1, 1).start()
            moved_copy(1, 0).start()
            if square:
                pl.semaphore_wait(corner_sem, 1)
        kv_copy(0, k).start()
    for k in range(1, ctx_count):
        kv_copy(first_late, k).start()

    first_cols = pl.ds(0, moved_first)
    load(0, moved_first, q_buf.at[:, :, first_cols], local_sem.at[1])
    for g in range(1, moved):
        load_kv(g, kv_buf.at[g, :, :, my_rows, :], local_sem.at[0])
    for copy in scalars:
        copy.wait()

    def ends_of(sequence):
        ends = []
        total_length = 0
        for d in range(docs):
            total_length = total_length + lengths_ref[sequence, d]
            ends.append(total_length)
        return ends

    own_ends = ends_of(dp_index)

    def identity_of(place, slots, settled):
        first = place < span
        position = jnp.where(
            first, order_ref[slots[0]] * span, order_ref[slots[1]] * span - span
        ) + place
        partners = dest_ref[0, slots[0]], dest_ref[0, slots[1]]
        counted = jnp.where(first, partners[0] * docs, partners[1] * docs)
        if settled:
            ends = [jnp.where(first, *pair) for pair in zip(ends_of(partners[0]), ends_of(partners[1]))]
        else:
            ends = own_ends
        for end in ends:
            counted = counted + (position >= end).astype(jnp.int32)
        return position, counted

    query_place = lax.broadcasted_iota(jnp.int32, (2 * span, 2 * span), 0)
    key_place = lax.broadcasted_iota(jnp.int32, (1, 2 * span), 1)

    def build_bias(settled, early_target, late_target):
        query_position, query_document = identity_of(query_place, (2 * me, 2 * me + 1), settled)
        for half in range(2):
            for b in range(0, ctx_count, 2):
                key_position, key_document = identity_of(
                    key_place, (2 * b + half, 2 * b + 2 + half), settled
                )
                visible = (key_document == query_document) & (key_position <= query_position)
                mask = jnp.where(visible, 0.0, MASK_FLOOR)
                if half == 0:
                    early_target[:, b * span:(b + 2) * span] = mask[:span]
                late_target[:, half * keys + b * span:half * keys + (b + 2) * span] = mask[span:]

    build_bias(False, early_bias, late_bias)
    loaded(later_kv, local_sem.at[0])
    for g in range(1, moved):
        for k in range(1, ctx_count):
            kv_copy(g, k).start()
    build_bias(True, settled_early_bias, settled_late_bias)
    loaded(q_buf.at[:, :, first_cols], local_sem.at[1])

    def settle_rows(half, kept, lower, upper):
        source = dest_ref[0, 2 * me + half]
        chosen = jnp.where(
            source == below, lower.astype(jnp.float32),
            jnp.where(source == above, upper.astype(jnp.float32), kept.astype(jnp.float32)),
        )
        return chosen.astype(jnp.bfloat16)

    odd = lax.rem(dp_index, 2)
    closing = (dp_index == 0) | (dp_index == dp_count - 1)
    links_before = lax.div(jnp.where(odd == 1, dp_index, dp_count - 2 - dp_index), 2)
    holds = jnp.logical_not(closing) & (links_before < dp_count // 2 - 2)

    def send(start, count, part="all"):
        some = pl.ds(start, count)
        for up in range(2):
            copy = pltpu.make_async_remote_copy(
                src_ref=own.at[some],
                dst_ref=arrived.at[up, some],
                send_sem=out_send.at[up],
                recv_sem=out_recv.at[batch_of(start, starts)],
                device_id={"dp": above if up else below},
                device_id_type=MESH,
            )
            if part == "all":
                copy.start()
            else:
                held = (odd == up) & holds
                pl.when(held if part == "held" else jnp.logical_not(held))(copy.start)

    exponent_scale = math.log2(math.e) / math.sqrt(HEAD_SIZE)

    def attend(queries, g, half, mask, between=None):
        width = keys * (1 + half)
        stacked = jnp.concatenate(queries, axis=0)
        key_rows, value_rows = (
            kv_buf[g, part].reshape(width, HEAD_SIZE) if half else kv_buf[g, part, 0]
            for part in range(2)
        )
        scores = lax.dot_general(
            stacked, key_rows, (((1,), (1,)), ((), ())), preferred_element_type=jnp.float32
        )
        if between is not None:
            between()
        scores = scores.reshape(len(queries), span, width) + mask[...][None]
        scores = scores.reshape(len(queries) * span, width)
        row_max = jnp.max(scores, axis=1, keepdims=True)
        weights = jnp.exp2((scores - row_max) * exponent_scale)
        total = jnp.sum(weights, axis=1, keepdims=True)
        mixed = jnp.dot(
            weights.astype(jnp.bfloat16), value_rows, preferred_element_type=jnp.float32
        )
        mixed = (mixed / total).astype(jnp.bfloat16)
        return [mixed[j * span:(j + 1) * span] for j in range(len(queries))]

    def head_cols(first, j):
        return pl.ds(pl.multiple_of(first + j * HEAD_SIZE, HEAD_SIZE), HEAD_SIZE)

    for g in range(moved):
        for half in range(2):
            if g == 0 or half == 0:
                index = first_late if g == 0 and half else g
                wait_bytes(others_of(index), kv_recv.at[index])

            phase = 2 * g + half
            before = phase * group_units

            def one_unit(i, carry):
                unit = before + i
                first = (g * group_units + i) * unit_cols

                def send_done():
                    if g > 0:
                        if phase > 2:
                            pl.when(i == 0)(lambda: send(before - group_units, group_units))
                        return
                    for n in range(group_units):
                        if before + n > 0:
                            pl.when(i == n)(lambda: send(before + n - 1, 1, "prompt"))

                heads = attend(
                    [q_buf[half, :, head_cols(first, j)] for j in range(UNIT_HEADS)],
                    g, half, late_bias if half else early_bias, send_done,
                )
                for j, head in enumerate(heads):
                    own[unit, :, j * HEAD_SIZE:(j + 1) * HEAD_SIZE] = head
                return carry

            if g == moved - 1 and half == 0:
                for k in range(1, ctx_count):
                    kv_copy(moved, k).start()
            lax.fori_loop(0, group_units, one_unit, 0)
            if phase == 1:
                send(before + group_units - 1, 1, "prompt")
                send(0, before + group_units, "held")
        if g == max(moved - 2, 0):
            wait_bytes(moved_kv, moved_recv.at[0])
            for part in range(2):
                for half in range(2):
                    kv_buf[moved, part, half, my_rows, :] = settle_rows(
                        half, own_kv[part, half], moved_kv[1, part, half], moved_kv[0, part, half]
                    )
    send(units - group_units, group_units)

    wait_bytes(moved_q, moved_recv.at[1])
    wait_bytes(others_of(moved), kv_recv.at[moved])

    for half in range(2):
        def one_moved(i, carry):
            queries = []
            for j in range(UNIT_HEADS):
                inner = head_cols(i * unit_cols, j)
                queries.append(settle_rows(
                    half, q_buf[half, :, head_cols(moved_first + i * unit_cols, j)],
                    moved_q[1, half, :, inner], moved_q[0, half, :, inner],
                ))
            heads = attend(queries, moved, half, settled_late_bias if half else settled_early_bias)
            for j, head in enumerate(heads):
                out_ref[half, :, head_cols(moved_first + i * unit_cols, j)] = head
            return carry

        lax.fori_loop(0, group_units, one_moved, 0)

    moved_units = (4 * QUERIES_PER_KV + 8) * HEAD_SIZE // unit_cols
    wait_bytes(own.at[pl.ds(0, moved_units)], moved_send)
    wait_bytes(kv_buf.at[:, :, :, pl.ds(0, (ctx_count - 1) * span), :], kv_send)

    def settle(unit, carry):
        half = lax.rem(lax.div(unit, group_units), 2)
        first = (lax.div(unit, 2 * group_units) * group_units + lax.rem(unit, group_units)) * unit_cols
        for j in range(UNIT_HEADS):
            part = pl.ds(j * HEAD_SIZE, HEAD_SIZE)
            out_ref[half, :, head_cols(first, j)] = settle_rows(
                half, own[unit, :, part], arrived[1, unit, :, part], arrived[0, unit, :, part]
            )
        return carry

    for batch, (start, size) in enumerate(zip(starts, batches)):
        if batch == len(batches) - 1:
            for up in range(2):
                wait_bytes(own, out_send.at[up])
        wait_bytes(arrived.at[:, pl.ds(start, size)], out_recv.at[batch])
        lax.fori_loop(start, start + size, settle, 0)


def place_kernel(settled_ref, out_ref, sem):
    rows = settled_ref.shape[1] // (PLACE_PARTS // 2)
    copies = [
        pltpu.make_async_copy(
            settled_ref.at[half, pl.ds(i * rows, rows), :],
            out_ref.at[half, pl.ds(i * rows, rows), :],
            sem,
        )
        for half in range(2) for i in range(PLACE_PARTS // 2)
    ]
    for copy in copies:
        copy.start()
    pltpu.make_async_copy(settled_ref, out_ref, sem).wait()


def on_device(dp_count, ctx_count, qkv, dest, order, lengths):
    span = qkv.shape[1] // 2
    query_width = QUERY_HEADS * HEAD_SIZE
    group_width = QUERIES_PER_KV * HEAD_SIZE
    units = 2 * (QUERY_HEADS - QUERIES_PER_KV) // UNIT_HEADS
    unit_shape = (units, span, UNIT_HEADS * HEAD_SIZE)
    keys = ctx_count * span
    qkv = qkv.reshape(2, span, qkv.shape[2])
    qkv, dest, order, lengths = (
        pltpu.with_memory_space_constraint(array, pltpu.HBM)
        for array in (qkv, dest, order, lengths)
    )
    settled = pl.pallas_call(
        functools.partial(kernel, dp_count, ctx_count),
        out_shape=pltpu.VMEM((2, span, query_width), jnp.bfloat16),
        in_specs=[pl.BlockSpec(memory_space=pltpu.HBM)] * 4,
        out_specs=pl.BlockSpec(memory_space=pltpu.VMEM),
        scratch_shapes=[
            pltpu.SMEM(dest.shape, jnp.int32),
            pltpu.SMEM(order.shape, jnp.int32),
            pltpu.SMEM(lengths.shape, jnp.int32),
            pltpu.VMEM((2, span, query_width), jnp.bfloat16),
            pltpu.VMEM((KEY_VALUE_HEADS, 2, 2, keys, HEAD_SIZE), jnp.bfloat16),
            pltpu.VMEM((span, keys), jnp.float32),
            pltpu.VMEM((span, 2 * keys), jnp.float32),
            pltpu.VMEM((span, keys), jnp.float32),
            pltpu.VMEM((span, 2 * keys), jnp.float32),
            pltpu.VMEM(unit_shape, jnp.bfloat16),
            pltpu.VMEM((2, *unit_shape), jnp.bfloat16),
            pltpu.VMEM((2, 2, span, group_width), jnp.bfloat16),
            pltpu.VMEM((2, 2, 2, span, HEAD_SIZE), jnp.bfloat16),
            pltpu.VMEM((2, 2, span, HEAD_SIZE), jnp.bfloat16),
            pltpu.SemaphoreType.DMA((3,)),
            pltpu.SemaphoreType.DMA,
            pltpu.SemaphoreType.DMA((KEY_VALUE_HEADS + 1,)),
            pltpu.SemaphoreType.DMA((2,)),
            pltpu.SemaphoreType.DMA((len(batches_of(units)),)),
            pltpu.SemaphoreType.DMA,
            pltpu.SemaphoreType.DMA((2,)),
            pltpu.SemaphoreType.REGULAR,
        ],
        compiler_params=pltpu.CompilerParams(collective_id=0, has_side_effects=True,
            vmem_limit_bytes=40 << 20),
    )(qkv, dest, order, lengths)
    placed = pl.pallas_call(
        place_kernel,
        out_shape=jax.ShapeDtypeStruct((2, span, query_width), jnp.bfloat16),
        in_specs=[pl.BlockSpec(memory_space=pltpu.VMEM)],
        out_specs=pl.BlockSpec(memory_space=pltpu.HBM),
        scratch_shapes=[pltpu.SemaphoreType.DMA],
        compiler_params=pltpu.CompilerParams(vmem_limit_bytes=8 << 20),
    )(settled)
    return placed.reshape(1, 2 * span, query_width)


def solution(mesh):
    return jax.shard_map(
        functools.partial(on_device, mesh.shape["dp"], mesh.shape["ctx"]),
        mesh=mesh,
        in_specs=(P("dp", "ctx", None), P("dp", None), P(), P()),
        out_specs=P("dp", "ctx", None),
        check_vma=False,
    )
```

```python
import functools
import math

import jax
import jax.numpy as jnp
from jax import lax
from jax.experimental import pallas as pl
from jax.experimental.pallas import tpu as pltpu
from jax.sharding import PartitionSpec as P

QUERY_HEADS = 32
KEY_VALUE_HEADS = 4
HEAD_SIZE = 128
QUERIES_PER_KV = 8
UNIT_HEADS = 4
PLACE_PARTS = 4
LAST_BATCHES = (2,)

MASK_FLOOR = -1e30
MESH = pl.DeviceIdType.MESH


def batches_of(units):
    return (units - sum(LAST_BATCHES), *LAST_BATCHES)


def batch_of(unit, starts):
    return sum(unit >= start for start in starts[1:])


def kernel(
    dp_count, ctx_count,
    qkv_ref, dest_hbm, order_hbm, lengths_hbm,
    out_ref,
    dest_ref, order_ref, lengths_ref, q_buf, kv_buf,
    early_bias, late_bias, settled_early_bias, settled_late_bias,
    own, arrived, moved_q, moved_kv, own_kv,
    local_sem, kv_send, kv_recv, out_send, out_recv, moved_send, moved_recv, corner_sem,
):
    dp_index = lax.axis_index("dp")
    me = lax.axis_index("ctx")
    above = lax.rem(dp_index + 1, dp_count)
    below = lax.rem(dp_index + dp_count - 1, dp_count)
    span = qkv_ref.shape[1]
    keys = ctx_count * span
    docs = lengths_ref.shape[1]
    query_width = QUERY_HEADS * HEAD_SIZE
    unit_cols = UNIT_HEADS * HEAD_SIZE
    moved = KEY_VALUE_HEADS - 1
    group_units = QUERIES_PER_KV // UNIT_HEADS
    units = moved * 2 * group_units
    batches = batches_of(units)
    starts = [sum(batches[:n]) for n in range(len(batches))]
    moved_first = moved * QUERIES_PER_KV * HEAD_SIZE
    moved_cols = pl.ds(moved_first, QUERIES_PER_KV * HEAD_SIZE)
    my_rows = pl.ds(pl.multiple_of(me * span, span), span)

    square = ctx_count == 4

    def target_of(k):
        if square:
            return (me + 1 - 2 * lax.rem(me, 2), lax.rem(me + 2, 4), 3 - me)[k - 1]
        return lax.rem(me + k, ctx_count)

    def origin_of(k):
        return target_of(k) if square else lax.rem(me + ctx_count - k, ctx_count)

    barrier = pltpu.get_barrier_semaphore()
    pl.semaphore_signal(barrier, inc=1, device_id={"dp": above}, device_id_type=MESH)
    pl.semaphore_signal(barrier, inc=1, device_id={"dp": below}, device_id_type=MESH)
    for k in range(1, 3 if square else ctx_count):
        pl.semaphore_signal(barrier, inc=1, device_id={"ctx": target_of(k)}, device_id_type=MESH)
    scalars = [
        pltpu.make_async_copy(source, target, sem)
        for source, target, sem in (
            (dest_hbm, dest_ref, out_send.at[0]),
            (order_hbm, order_ref, out_send.at[1]),
            (lengths_hbm, lengths_ref, local_sem.at[2]),
        )
    ]
    def load(first, width, target, sem):
        pltpu.make_async_copy(qkv_ref.at[:, :, pl.ds(first, width)], target, sem).start()

    def loaded(target, sem):
        pltpu.make_async_copy(target, target, sem).wait()

    def load_kv(g, target, sem):
        for part in range(2):
            first = query_width + (part * KEY_VALUE_HEADS + g) * HEAD_SIZE
            load(first, HEAD_SIZE, target.at[part], sem)

    later_kv = kv_buf.at[pl.ds(1, moved - 1), :, :, my_rows, :]
    load_kv(moved, own_kv, kv_send)
    load_kv(0, kv_buf.at[0, :, :, my_rows, :], local_sem.at[0])
    load(moved_first, query_width - moved_first, q_buf.at[:, :, moved_cols], local_sem.at[1])
    for copy in scalars:
        copy.start()

    pl.semaphore_wait(barrier, 4 if square else ctx_count + 1)
    if square:
        pl.semaphore_signal(corner_sem, inc=1, device_id={"ctx": target_of(1)}, device_id_type=MESH)

    first_late = KEY_VALUE_HEADS

    def block_of(index, rows):
        if index == 0:
            return kv_buf.at[0, :, 0, rows, :]
        if index == first_late:
            return kv_buf.at[0, :, 1, rows, :]
        return kv_buf.at[index, :, :, rows, :]

    def kv_copy(index, k):
        block = block_of(index, my_rows)
        return pltpu.make_async_remote_copy(
            src_ref=block, dst_ref=block, send_sem=kv_send, recv_sem=kv_recv.at[index],
            device_id={"ctx": target_of(k)}, device_id_type=MESH,
        )

    def others_of(index):
        return block_of(index, pl.ds(0, (ctx_count - 1) * span))

    def wait_bytes(ref, sem):
        pltpu.make_async_copy(ref, ref, sem).wait()

    def moved_copy(kind, up):
        return pltpu.make_async_remote_copy(
            src_ref=q_buf.at[:, :, moved_cols] if kind else own_kv,
            dst_ref=(moved_q if kind else moved_kv).at[up],
            send_sem=moved_send,
            recv_sem=moved_recv.at[kind],
            device_id={"dp": above if up else below},
            device_id_type=MESH,
        )

    loaded(own_kv, kv_send)
    moved_copy(0, 1).start()
    moved_copy(0, 0).start()
    loaded(kv_buf.at[0, :, :, my_rows, :], local_sem.at[0])
    for k in range(1, ctx_count):
        if k == ctx_count - 1:
            loaded(q_buf.at[:, :, moved_cols], local_sem.at[1])
            moved_copy(1, 1).start()
            moved_copy(1, 0).start()
            if square:
                pl.semaphore_wait(corner_sem, 1)
        kv_copy(0, k).start()
    for k in range(1, ctx_count):
        kv_copy(first_late, k).start()

    first_cols = pl.ds(0, moved_first)
    load(0, moved_first, q_buf.at[:, :, first_cols], local_sem.at[1])
    for g in range(1, moved):
        load_kv(g, kv_buf.at[g, :, :, my_rows, :], local_sem.at[0])
    for copy in scalars:
        copy.wait()
    loaded(later_kv, local_sem.at[0])
    for g in range(1, moved):
        for k in range(1, ctx_count):
            kv_copy(g, k).start()

    def ends_of(sequence):
        ends = []
        total_length = 0
        for d in range(docs):
            total_length = total_length + lengths_ref[sequence, d]
            ends.append(total_length)
        return ends

    own_ends = ends_of(dp_index)

    def identity_of(place, slots, settled):
        first = place < span
        position = jnp.where(
            first, order_ref[slots[0]] * span, order_ref[slots[1]] * span - span
        ) + place
        partners = dest_ref[0, slots[0]], dest_ref[0, slots[1]]
        counted = jnp.where(first, partners[0] * docs, partners[1] * docs)
        if settled:
            ends = [jnp.where(first, *pair) for pair in zip(ends_of(partners[0]), ends_of(partners[1]))]
        else:
            ends = own_ends
        for end in ends:
            counted = counted + (position >= end).astype(jnp.int32)
        return position, counted

    query_place = lax.broadcasted_iota(jnp.int32, (2 * span, 2 * span), 0)
    key_place = lax.broadcasted_iota(jnp.int32, (1, 2 * span), 1)

    def build_bias(settled, early_target, late_target):
        query_position, query_document = identity_of(query_place, (2 * me, 2 * me + 1), settled)
        for half in range(2):
            for b in range(0, ctx_count, 2):
                key_position, key_document = identity_of(
                    key_place, (2 * b + half, 2 * b + 2 + half), settled
                )
                visible = (key_document == query_document) & (key_position <= query_position)
                mask = jnp.where(visible, 0.0, MASK_FLOOR)
                if half == 0:
                    early_target[:, b * span:(b + 2) * span] = mask[:span]
                late_target[:, half * keys + b * span:half * keys + (b + 2) * span] = mask[span:]

    build_bias(False, early_bias, late_bias)
    build_bias(True, settled_early_bias, settled_late_bias)
    loaded(q_buf.at[:, :, first_cols], local_sem.at[1])

    def settle_rows(half, kept, lower, upper):
        source = dest_ref[0, 2 * me + half]
        chosen = jnp.where(
            source == below, lower.astype(jnp.float32),
            jnp.where(source == above, upper.astype(jnp.float32), kept.astype(jnp.float32)),
        )
        return chosen.astype(jnp.bfloat16)

    odd = lax.rem(dp_index, 2)
    closing = (dp_index == 0) | (dp_index == dp_count - 1)
    links_before = lax.div(jnp.where(odd == 1, dp_index, dp_count - 2 - dp_index), 2)
    holds = jnp.logical_not(closing) & (links_before < dp_count // 2 - 2)

    def send(start, count, part="all"):
        some = pl.ds(start, count)
        for up in range(2):
            copy = pltpu.make_async_remote_copy(
                src_ref=own.at[some],
                dst_ref=arrived.at[up, some],
                send_sem=out_send.at[up],
                recv_sem=out_recv.at[batch_of(start, starts)],
                device_id={"dp": above if up else below},
                device_id_type=MESH,
            )
            if part == "all":
                copy.start()
            else:
                held = (odd == up) & holds
                pl.when(held if part == "held" else jnp.logical_not(held))(copy.start)

    exponent_scale = math.log2(math.e) / math.sqrt(HEAD_SIZE)

    def attend(queries, g, half, mask, between=None):
        width = keys * (1 + half)
        stacked = jnp.concatenate(queries, axis=0)
        key_rows, value_rows = (
            kv_buf[g, part].reshape(width, HEAD_SIZE) if half else kv_buf[g, part, 0]
            for part in range(2)
        )
        scores = lax.dot_general(
            stacked, key_rows, (((1,), (1,)), ((), ())), preferred_element_type=jnp.float32
        )
        if between is not None:
            between()
        scores = scores.reshape(len(queries), span, width) + mask[...][None]
        scores = scores.reshape(len(queries) * span, width)
        row_max = jnp.max(scores, axis=1, keepdims=True)
        weights = jnp.exp2((scores - row_max) * exponent_scale)
        total = jnp.sum(weights, axis=1, keepdims=True)
        mixed = jnp.dot(
            weights.astype(jnp.bfloat16), value_rows, preferred_element_type=jnp.float32
        )
        mixed = (mixed / total).astype(jnp.bfloat16)
        return [mixed[j * span:(j + 1) * span] for j in range(len(queries))]

    def head_cols(first, j):
        return pl.ds(pl.multiple_of(first + j * HEAD_SIZE, HEAD_SIZE), HEAD_SIZE)

    for g in range(moved):
        for half in range(2):
            if g == 0 or half == 0:
                index = first_late if g == 0 and half else g
                wait_bytes(others_of(index), kv_recv.at[index])

            phase = 2 * g + half
            before = phase * group_units

            def one_unit(i, carry):
                unit = before + i
                first = (g * group_units + i) * unit_cols

                def send_done():
                    if g > 0:
                        if phase > 2:
                            pl.when(i == 0)(lambda: send(before - group_units, group_units))
                        return
                    for n in range(group_units):
                        if before + n > 0:
                            pl.when(i == n)(lambda: send(before + n - 1, 1, "prompt"))

                heads = attend(
                    [q_buf[half, :, head_cols(first, j)] for j in range(UNIT_HEADS)],
                    g, half, late_bias if half else early_bias, send_done,
                )
                for j, head in enumerate(heads):
                    own[unit, :, j * HEAD_SIZE:(j + 1) * HEAD_SIZE] = head
                return carry

            if g == moved - 1 and half == 0:
                for k in range(1, ctx_count):
                    kv_copy(moved, k).start()
            lax.fori_loop(0, group_units, one_unit, 0)
            if phase == 1:
                send(before + group_units - 1, 1, "prompt")
                send(0, before + group_units, "held")
        if g == max(moved - 2, 0):
            wait_bytes(moved_kv, moved_recv.at[0])
            for part in range(2):
                for half in range(2):
                    kv_buf[moved, part, half, my_rows, :] = settle_rows(
                        half, own_kv[part, half], moved_kv[1, part, half], moved_kv[0, part, half]
                    )
    send(units - group_units, group_units)

    wait_bytes(moved_q, moved_recv.at[1])
    wait_bytes(others_of(moved), kv_recv.at[moved])

    for half in range(2):
        def one_moved(i, carry):
            queries = []
            for j in range(UNIT_HEADS):
                inner = head_cols(i * unit_cols, j)
                queries.append(settle_rows(
                    half, q_buf[half, :, head_cols(moved_first + i * unit_cols, j)],
                    moved_q[1, half, :, inner], moved_q[0, half, :, inner],
                ))
            heads = attend(queries, moved, half, settled_late_bias if half else settled_early_bias)
            for j, head in enumerate(heads):
                out_ref[half, :, head_cols(moved_first + i * unit_cols, j)] = head
            return carry

        lax.fori_loop(0, group_units, one_moved, 0)

    moved_units = (4 * QUERIES_PER_KV + 8) * HEAD_SIZE // unit_cols
    wait_bytes(own.at[pl.ds(0, moved_units)], moved_send)
    wait_bytes(kv_buf.at[:, :, :, pl.ds(0, (ctx_count - 1) * span), :], kv_send)

    def settle(unit, carry):
        half = lax.rem(lax.div(unit, group_units), 2)
        first = (lax.div(unit, 2 * group_units) * group_units + lax.rem(unit, group_units)) * unit_cols
        for j in range(UNIT_HEADS):
            part = pl.ds(j * HEAD_SIZE, HEAD_SIZE)
            out_ref[half, :, head_cols(first, j)] = settle_rows(
                half, own[unit, :, part], arrived[1, unit, :, part], arrived[0, unit, :, part]
            )
        return carry

    for batch, (start, size) in enumerate(zip(starts, batches)):
        if batch == len(batches) - 1:
            for up in range(2):
                wait_bytes(own, out_send.at[up])
        wait_bytes(arrived.at[:, pl.ds(start, size)], out_recv.at[batch])
        lax.fori_loop(start, start + size, settle, 0)


def place_kernel(settled_ref, out_ref, sem):
    rows = settled_ref.shape[1] // (PLACE_PARTS // 2)
    copies = [
        pltpu.make_async_copy(
            settled_ref.at[half, pl.ds(i * rows, rows), :],
            out_ref.at[half, pl.ds(i * rows, rows), :],
            sem,
        )
        for half in range(2) for i in range(PLACE_PARTS // 2)
    ]
    for copy in copies:
        copy.start()
    pltpu.make_async_copy(settled_ref, out_ref, sem).wait()


def on_device(dp_count, ctx_count, qkv, dest, order, lengths):
    span = qkv.shape[1] // 2
    query_width = QUERY_HEADS * HEAD_SIZE
    group_width = QUERIES_PER_KV * HEAD_SIZE
    units = 2 * (QUERY_HEADS - QUERIES_PER_KV) // UNIT_HEADS
    unit_shape = (units, span, UNIT_HEADS * HEAD_SIZE)
    keys = ctx_count * span
    qkv = qkv.reshape(2, span, qkv.shape[2])
    qkv, dest, order, lengths = (
        pltpu.with_memory_space_constraint(array, pltpu.HBM)
        for array in (qkv, dest, order, lengths)
    )
    settled = pl.pallas_call(
        functools.partial(kernel, dp_count, ctx_count),
        out_shape=pltpu.VMEM((2, span, query_width), jnp.bfloat16),
        in_specs=[pl.BlockSpec(memory_space=pltpu.HBM)] * 4,
        out_specs=pl.BlockSpec(memory_space=pltpu.VMEM),
        scratch_shapes=[
            pltpu.SMEM(dest.shape, jnp.int32),
            pltpu.SMEM(order.shape, jnp.int32),
            pltpu.SMEM(lengths.shape, jnp.int32),
            pltpu.VMEM((2, span, query_width), jnp.bfloat16),
            pltpu.VMEM((KEY_VALUE_HEADS, 2, 2, keys, HEAD_SIZE), jnp.bfloat16),
            pltpu.VMEM((span, keys), jnp.float32),
            pltpu.VMEM((span, 2 * keys), jnp.float32),
            pltpu.VMEM((span, keys), jnp.float32),
            pltpu.VMEM((span, 2 * keys), jnp.float32),
            pltpu.VMEM(unit_shape, jnp.bfloat16),
            pltpu.VMEM((2, *unit_shape), jnp.bfloat16),
            pltpu.VMEM((2, 2, span, group_width), jnp.bfloat16),
            pltpu.VMEM((2, 2, 2, span, HEAD_SIZE), jnp.bfloat16),
            pltpu.VMEM((2, 2, span, HEAD_SIZE), jnp.bfloat16),
            pltpu.SemaphoreType.DMA((3,)),
            pltpu.SemaphoreType.DMA,
            pltpu.SemaphoreType.DMA((KEY_VALUE_HEADS + 1,)),
            pltpu.SemaphoreType.DMA((2,)),
            pltpu.SemaphoreType.DMA((len(batches_of(units)),)),
            pltpu.SemaphoreType.DMA,
            pltpu.SemaphoreType.DMA((2,)),
            pltpu.SemaphoreType.REGULAR,
        ],
        compiler_params=pltpu.CompilerParams(collective_id=0, has_side_effects=True,
            vmem_limit_bytes=40 << 20),
    )(qkv, dest, order, lengths)
    placed = pl.pallas_call(
        place_kernel,
        out_shape=jax.ShapeDtypeStruct((2, span, query_width), jnp.bfloat16),
        in_specs=[pl.BlockSpec(memory_space=pltpu.VMEM)],
        out_specs=pl.BlockSpec(memory_space=pltpu.HBM),
        scratch_shapes=[pltpu.SemaphoreType.DMA],
        compiler_params=pltpu.CompilerParams(vmem_limit_bytes=8 << 20),
    )(settled)
    return placed.reshape(1, 2 * span, query_width)


def solution(mesh):
    return jax.shard_map(
        functools.partial(on_device, mesh.shape["dp"], mesh.shape["ctx"]),
        mesh=mesh,
        in_specs=(P("dp", "ctx", None), P("dp", None), P(), P()),
        out_specs=P("dp", "ctx", None),
        check_vma=False,
    )
```
